32 devices in a mesh: frame: 2 (over x), height: 4 (over z), width: 4 (over y, core).
Axes of the slice: x: 2, y: 2, z: 4, core: 2. Of those that a mesh axis runs over, the one named last changes fastest.
Arguments:
- activations: bfloat16 [8, 64, 128, 256], P('frame', 'height', 'width'), may hold values from -6 to 6
- out_grad: bfloat16 [8, 64, 128, 256], P('frame', 'height', 'width'), may hold values from -40 to 40
- kernel: bfloat16 [6912, 256], P(('frame', 'height', 'width')), may hold values from -5 to 5
- damping: float32 [], replicated, may hold values from 0.02 to 0.2
Outputs:
- input_grad: bfloat16 [8, 64, 128, 256], P('frame', 'height', 'width')
- new_kernel: bfloat16 [6912, 256], replicated
The draws below stay inside these ranges and needn't reach their ends.
All inputs are finite; a program needn't handle non-finite values.
Results may differ from the reference program's by a relative error of at most 0.001.
Values may be sent and summed in bfloat16 or wider, within the bound.
No kernel may reach another device: no remote copies, remote signals or barrier semaphores. Data moves between devices by JAX's collectives and lax.ppermute only.
A program may use at most 192 MiB of HBM per device.

```python
import math
import jax
import jax.numpy as jnp
from jax import lax

C = 256
ITERS = 12
NF = 8
NH = 64
NW = 128
KROWS = 6912


def draw_out_grad(key, part):
    first, second = jax.random.split(jax.random.fold_in(key, 7))
    scales = jnp.exp(jax.random.uniform(first, (C,), jnp.float32, math.log(0.1), math.log(10.0)))
    base = jnp.clip(jax.random.normal(second, (NF, NH, NW, C), jnp.float32), -4.0, 4.0)
    return (base * scales).astype(jnp.bfloat16)


def shard_levels(rng, dims, cuts, smallest, top_value):
    def one(position, blocks):
        heights = jax.random.uniform(jax.random.fold_in(jax.random.fold_in(rng, 6), position), (blocks,), jnp.float32, smallest / len(cuts), top_value / len(cuts))
        return jnp.repeat(jnp.exp(heights), dims[position] // blocks).reshape((-1,) + (1,) * (len(dims) - position - 1))

    loudness = one(*cuts[0])
    for cut in cuts[1:]:
        loudness = loudness * one(*cut)
    return loudness


def normal_values(own_key, extent, deviation, bound, shards=(), kind=jnp.bfloat16):
    level = shard_levels(own_key, extent, shards, -0.22, 0.18) if shards else 1.0
    drawn = jax.random.normal(own_key, extent, jnp.float32) * deviation * level
    return jnp.minimum(jnp.maximum(drawn, -bound), bound).astype(kind)


def setup_inputs(seed: int = 0) -> dict:
    key_of = jax.random.split(jax.random.key(seed), 5)
    return {
        "activations": normal_values(key_of[0], (NF, NH, NW, C), 1.0, 6.0, ((0, 2), (1, 4), (2, 4))),
        "out_grad": draw_out_grad(jax.random.fold_in(key_of[4], 71), 0),
        "kernel": normal_values(key_of[2], (KROWS, C), 1.0, 5.0, ((0, 32),)),
        "damping": jnp.clip(jnp.exp(jax.random.uniform(key_of[3], (), jnp.float32, math.log(0.02), math.log(0.2))), 0.02, 0.2),
    }


def newton_root(gram, damping):
    order = gram.shape[0]
    identity = jnp.eye(order, dtype=jnp.float32)
    factor = gram + damping * (jnp.trace(gram) / order) * identity
    start_scale = 2.5 / jnp.sqrt(jnp.sum(factor * factor))
    inverse_root = jnp.sqrt(jnp.sqrt(start_scale)) * identity
    matrix = start_scale * factor
    for step in range(ITERS):
        middle = (5.0 * identity - matrix) / 4.0
        inverse_root = jnp.dot(inverse_root, middle, precision=lax.Precision.HIGHEST)
        square = jnp.dot(middle, middle, precision=lax.Precision.HIGHEST)
        matrix = jnp.dot(square, jnp.dot(square, matrix, precision=lax.Precision.HIGHEST), precision=lax.Precision.HIGHEST)
    return inverse_root

def frame_padded(volume, index):
    frames = volume.shape[0]
    safe = jnp.clip(index, 0, frames - 1).astype(jnp.int32)
    piece = lax.dynamic_index_in_dim(volume, safe, 0, keepdims=False)
    valid = jnp.logical_and(index >= 0, index < frames)
    piece = jnp.where(valid, piece, jnp.zeros_like(piece))
    return jnp.pad(piece, ((1, 1), (1, 1), (0, 0)))

def reference(activations, out_grad, kernel, damping):
    frames, height, width, chans = activations.shape
    count = height * width
    krows = kernel.shape[0]

    def one_frame(carry, index):
        own_grad = lax.dynamic_index_in_dim(out_grad, index.astype(jnp.int32), 0, keepdims=False).reshape(count, chans)
        pieces = []
        total = jnp.zeros((count, chans), jnp.float32)
        for tap_f in range(3):
            slab_in = frame_padded(activations, index + tap_f - 1)
            slab_grad = frame_padded(out_grad, index + 1 - tap_f)
            for tap_h in range(3):
                for tap_w in range(3):
                    tap = 9 * tap_f + 3 * tap_h + tap_w
                    shifted = slab_in[tap_h:tap_h + height, tap_w:tap_w + width].reshape(count, chans)
                    pieces.append(lax.dot_general(shifted, own_grad, (((0,), (0,)), ((), ())), preferred_element_type=jnp.float32))
                    back = slab_grad[2 - tap_h:2 - tap_h + height, 2 - tap_w:2 - tap_w + width].reshape(count, chans)
                    total = total + jnp.dot(back, kernel[tap * chans:(tap + 1) * chans], preferred_element_type=jnp.float32)
        frame_grad = (total / jnp.sqrt(jnp.float32(krows))).astype(jnp.bfloat16).reshape(height, width, chans)
        return (carry + jnp.concatenate(pieces, 0), frame_grad)
    start = jnp.zeros((krows, chans), jnp.float32)
    kernel_grad, input_grad = lax.scan(one_frame, start, jnp.arange(frames, dtype=jnp.int32))
    gram = lax.dot_general(kernel_grad, kernel_grad, (((0,), (0,)), ((), ())), precision=lax.Precision.HIGHEST)
    inverse_root = newton_root(gram, damping)
    direction = jnp.dot(kernel_grad, inverse_root, precision=lax.Precision.HIGHEST)
    size = jnp.sqrt(jnp.mean(direction * direction) + 1e-06)
    new_kernel = (kernel.astype(jnp.float32) - 0.5 * direction / size).astype(jnp.bfloat16)
    return (input_grad, new_kernel)
```

```python
import jax
import jax.numpy as jnp
from jax import lax
from jax.sharding import PartitionSpec as P

ITERS = 12
AXES = ("frame", "height", "width")
HIGHEST = lax.Precision.HIGHEST


def bits_of(axis):
    size = lax.axis_size(axis)
    assert size & (size - 1) == 0
    return [(axis, k) for k in range(size.bit_length() - 1)]


def upper(stage):
    axis, k = stage
    return (lax.axis_index(axis) >> k) & 1


def swap(value, stage):
    axis, k = stage
    return lax.ppermute(value, axis, [(i, i ^ (1 << k)) for i in range(lax.axis_size(axis))])


def halve(value, stage):
    half = value.shape[0] // 2
    up = upper(stage)
    got = swap(lax.dynamic_slice_in_dim(value, (1 - up) * half, half), stage)
    return lax.dynamic_slice_in_dim(value, up * half, half) + got


def double(value, stage):
    got = swap(value, stage)
    up = upper(stage) == 1
    return jnp.concatenate([jnp.where(up, got, value), jnp.where(up, value, got)], 0)


def with_halo(cells, axis, dim):
    count = lax.axis_size(axis)
    head = lax.slice_in_dim(cells, 0, 1, axis=dim)
    tail = lax.slice_in_dim(cells, cells.shape[dim] - 1, cells.shape[dim], axis=dim)
    if count == 2:
        first = lax.axis_index(axis) == 0
        got = lax.ppermute(jnp.where(first, tail, head), axis, [(0, 1), (1, 0)])
        none = jnp.zeros_like(got)
        before, after = jnp.where(first, none, got), jnp.where(first, got, none)
    else:
        before = lax.ppermute(tail, axis, [(i, i + 1) for i in range(count - 1)])
        after = lax.ppermute(head, axis, [(i + 1, i) for i in range(count - 1)])
    return jnp.concatenate([before, cells, after], axis=dim)


def gathered(rows, stages):
    own = rows.shape
    value = rows[None]
    for stage in stages:
        value = double(value, stage)
    order = stages[::-1]
    want = [s for axis in AXES for s in reversed(bits_of(axis))]
    value = value.reshape((2,) * len(order) + own)
    value = value.transpose([order.index(s) for s in want] + [len(order) + d for d in range(len(own))])
    return value.reshape((-1,) + own[1:])


def newton_root(gram, damping):
    order = gram.shape[0]
    identity = jnp.eye(order, dtype=jnp.float32)
    factor = gram + damping * (jnp.trace(gram) / order) * identity
    start_scale = 2.5 / jnp.sqrt(jnp.sum(factor * factor))
    inverse_root = jnp.sqrt(jnp.sqrt(start_scale)) * identity
    matrix = start_scale * factor
    for step in range(ITERS):
        middle = (5.0 * identity - matrix) / 4.0
        inverse_root = jnp.dot(inverse_root, middle, precision=HIGHEST)
        square = jnp.dot(middle, middle, precision=HIGHEST)
        matrix = jnp.dot(square, jnp.dot(square, matrix, precision=HIGHEST), precision=HIGHEST)
    return inverse_root


def on_device(activations, out_grad, kernel, damping):
    frames, height, width, chans = activations.shape
    count = frames * height * width
    near = bits_of("width")[:1]
    rest = bits_of("width")[1:]
    frame_bits, height_bits = bits_of("frame"), bits_of("height")
    krows = kernel.shape[0] * lax.axis_size(AXES)

    full_kernel = gathered(kernel, height_bits[::-1] + frame_bits + rest + near)

    flat = with_halo(with_halo(out_grad, "height", 1), "width", 2)
    padded = with_halo(flat, "frame", 0)
    flat_in = activations.reshape(count, chans)

    def piece(tap):
        f, h, w = tap // 9, tap // 3 % 3, tap % 3
        source = flat if f == 1 else padded[2 - f : 2 - f + frames]
        back = source[:, 2 - h : 2 - h + height, 2 - w : 2 - w + width].reshape(count, chans)
        return lax.dot_general(
            flat_in, back, (((0,), (0,)), ((), ())), preferred_element_type=jnp.float32
        )

    order = list(range(9, 18)) + list(range(9)) + list(range(18, 27))
    pieces = [piece(t) for t in order]
    half = krows // 2
    mid = half // chans
    cut = half - mid * chans
    parts = [
        jnp.concatenate(pieces[:mid] + [pieces[mid][:cut]], 0),
        jnp.concatenate([pieces[mid][cut:]] + pieces[mid + 1 :], 0),
    ]
    ways = [near + frame_bits + rest, near + rest + frame_bits]
    for n, way in enumerate(ways):
        for stage in way:
            parts[n] = halve(parts[n], stage)
    rows = jnp.concatenate(parts, 0)
    for stage in height_bits:
        rows = halve(rows, stage)

    gram = lax.dot_general(rows, rows, (((0,), (0,)), ((), ())), precision=HIGHEST)
    for stage in near:
        gram = halve(gram, stage)
    for stage in frame_bits + rest + height_bits:
        gram = gram + swap(gram, stage)
    for stage in near:
        gram = double(gram, stage)

    for stage in height_bits[::-1]:
        rows = double(rows, stage)
    parts = list(jnp.split(rows, 2, 0))
    for n, way in enumerate(ways):
        for stage in way[::-1]:
            parts[n] = double(parts[n], stage)
    kernel_grad = jnp.concatenate(parts, 0)

    taps = full_kernel.reshape(3, 3, 3, chans, chans)
    total = lax.conv_general_dilated(
        padded[None],
        taps[::-1, ::-1, ::-1],
        (1, 1, 1),
        "VALID",
        dimension_numbers=("NDHWC", "DHWIO", "NDHWC"),
        preferred_element_type=jnp.float32,
    )[0]
    input_grad = (total / jnp.sqrt(jnp.float32(krows))).astype(jnp.bfloat16)

    inverse_root = newton_root(gram, damping)
    squares = jnp.sum(inverse_root * jnp.dot(gram, inverse_root, precision=HIGHEST))
    size = jnp.sqrt(squares / (krows * chans) + 1e-06)
    step = jnp.dot(kernel_grad, inverse_root * (0.5 / size), precision=lax.Precision.HIGH)
    step = step.reshape(27, chans, chans)
    step = jnp.concatenate([step[9:18], step[:9], step[18:]], 0).reshape(krows, chans)
    new_kernel = (full_kernel.astype(jnp.float32) - step).astype(jnp.bfloat16)
    return (input_grad, new_kernel)


def solution(mesh):
    placed = (
        P("frame", "height", "width", None),
        P("frame", "height", "width", None),
        P(("frame", "height", "width"), None),
        P(),
    )
    return jax.shard_map(
        on_device,
        mesh=mesh,
        in_specs=placed,
        out_specs=(P("frame", "height", "width", None), P()),
        check_vma=False,
    )
```

```python
import jax
import jax.numpy as jnp
from jax import lax
from jax.experimental import pallas as pl
from jax.experimental.pallas import tpu as pltpu
from jax.sharding import PartitionSpec as P

ITERS = 12
CENTRE_FIRST = list(range(9, 18)) + list(range(9)) + list(range(18, 27))
AXES = ("frame", "height", "width")
HIGHEST = lax.Precision.HIGHEST


def bits_of(axis):
    size = lax.axis_size(axis)
    assert size & (size - 1) == 0
    return [(axis, k) for k in range(size.bit_length() - 1)]


def upper(stage):
    axis, k = stage
    return (lax.axis_index(axis) >> k) & 1


def swap(value, stage):
    axis, k = stage
    return lax.ppermute(value, axis, [(i, i ^ (1 << k)) for i in range(lax.axis_size(axis))])


def short(value, scale):
    return (value * scale).astype(jnp.float16)


def halve(terms, stage, scale=None):
    half = terms[0].shape[0] // 2
    up = upper(stage)
    send = sum(lax.dynamic_slice_in_dim(t, (1 - up) * half, half) for t in terms)
    if scale is None:
        got = swap(send, stage)
    else:
        got = swap(short(send, scale[0]), stage).astype(jnp.float32) * scale[1]
    return [lax.dynamic_slice_in_dim(t, up * half, half) for t in terms] + [got]


def double(value, stage):
    got = swap(value, stage)
    up = upper(stage) == 1
    return jnp.concatenate([jnp.where(up, got, value), jnp.where(up, value, got)], 0)


def with_halo(cells, axis, dim):
    count = lax.axis_size(axis)
    head = lax.slice_in_dim(cells, 0, 1, axis=dim)
    tail = lax.slice_in_dim(cells, cells.shape[dim] - 1, cells.shape[dim], axis=dim)
    if count == 2:
        first = lax.axis_index(axis) == 0
        got = lax.ppermute(jnp.where(first, tail, head), axis, [(0, 1), (1, 0)])
        none = jnp.zeros_like(got)
        before, after = jnp.where(first, none, got), jnp.where(first, got, none)
    else:
        before = lax.ppermute(tail, axis, [(i, i + 1) for i in range(count - 1)])
        after = lax.ppermute(head, axis, [(i + 1, i) for i in range(count - 1)])
    return jnp.concatenate([before, cells, after], axis=dim)


def mul(left, right):
    return jnp.dot(left, right, precision=HIGHEST, preferred_element_type=jnp.float32)


def eye(order):
    rows = lax.broadcasted_iota(jnp.int32, (order, order), 0)
    return (rows == lax.broadcasted_iota(jnp.int32, (order, order), 1)).astype(jnp.float32)


def total_of(value):
    return jnp.sum(jnp.sum(value, 1, keepdims=True), 0, keepdims=True)


def newton_steps(matrix_ref, root_ref, steps):
    order = matrix_ref.shape[0]

    def step(_, carry):
        matrix = matrix_ref[...]
        middle = (5.0 * eye(order) - matrix) / 4.0
        both = mul(jnp.concatenate([middle, root_ref[...]], 0), middle)
        square = both[:order]
        root_ref[...] = both[order:]
        matrix_ref[...] = mul(square, mul(square, matrix))
        return carry

    lax.fori_loop(0, steps, step, 0)


def newton_start(gram, damping, steps):
    order = gram.shape[0]

    def body(damping_ref, gram_ref, matrix_ref, root_ref):
        gram = gram_ref[...]
        identity = eye(order)
        factor = gram + damping_ref[0, 0] * (total_of(gram * identity) / order) * identity
        scale = 2.5 / jnp.sqrt(total_of(factor * factor))
        root_ref[...] = jnp.sqrt(jnp.sqrt(scale)) * identity
        matrix_ref[...] = scale * factor
        newton_steps(matrix_ref, root_ref, steps)

    shape = jax.ShapeDtypeStruct(gram.shape, jnp.float32)
    return pl.pallas_call(
        body,
        in_specs=[pl.BlockSpec(memory_space=pltpu.SMEM), pl.BlockSpec(memory_space=pltpu.VMEM)],
        out_shape=(shape, shape),
        cost_estimate=pl.CostEstimate(flops=48 * steps * order**3, transcendentals=0, bytes_accessed=12 * order**2),
    )(damping.reshape(1, 1), gram)


def newton_end(gram, matrix, root, steps, entries):
    order = gram.shape[0]

    def body(gram_ref, matrix_in, root_in, out_ref, matrix_ref, root_ref):
        matrix_ref[...] = matrix_in[...]
        root_ref[...] = root_in[...]
        newton_steps(matrix_ref, root_ref, steps)
        root = root_ref[...]
        size = jnp.sqrt(total_of(root * mul(gram_ref[...], root)) / entries + 1e-06)
        out_ref[...] = root * (0.5 / size)

    shape = jax.ShapeDtypeStruct(gram.shape, jnp.float32)
    return pl.pallas_call(
        body,
        out_shape=shape,
        scratch_shapes=[pltpu.VMEM(gram.shape, jnp.float32)] * 2,
        cost_estimate=pl.CostEstimate(flops=48 * steps * order**3, transcendentals=0, bytes_accessed=16 * order**2),
    )(gram, matrix, root)


def run(activations, out_grad, kernel, damping):
    frames, height, width, chans = activations.shape
    count = frames * height * width
    near = bits_of("width")[:1]
    rest = bits_of("width")[1:]
    frame_bits, height_bits = bits_of("frame"), bits_of("height")
    rows_each = kernel.shape[0]
    krows = rows_each * lax.axis_size(AXES)
    ways = [near + frame_bits + rest, near + rest + frame_bits]

    flat = with_halo(with_halo(out_grad, "height", 1), "width", 2)
    padded = with_halo(flat, "frame", 0)

    top = jnp.max(jnp.abs(activations)).astype(jnp.float32) * jnp.max(jnp.abs(out_grad)).astype(jnp.float32)
    power = jnp.ceil(jnp.log2(jnp.maximum(top * count, 1e-30))).astype(jnp.bfloat16)
    extra = 16 - rows_each % 16
    tall = rows_each + extra
    gathered = jnp.concatenate([kernel, jnp.full((extra, chans), power, jnp.bfloat16)], 0)[None]
    for stage in height_bits[::-1]:
        gathered = double(gathered, stage)
    sides = []
    for p, way in enumerate(ways):
        side = gathered[..., p * (chans // 2) : (p + 1) * (chans // 2)]
        for stage in way[:0:-1]:
            side = double(side, stage)
        order = way[1:] + height_bits
        want = frame_bits + height_bits[::-1] + rest[::-1]
        side = side.reshape((2,) * len(order) + side.shape[1:])
        axes = [order.index(s) for s in want] + [len(order), len(order) + 1]
        sides.append(side.transpose(axes).reshape(-1, tall, chans // 2))
    full_kernel = jnp.concatenate(sides, 2)
    power = jnp.max(full_kernel[:, rows_each, 0])
    for stage in near:
        got = swap(full_kernel, stage)
        power = jnp.maximum(power, jnp.max(got[:, rows_each, 0]))
        up = upper(stage) == 1
        full_kernel = jnp.stack([jnp.where(up, got, full_kernel), jnp.where(up, full_kernel, got)], 1)
    full_kernel = full_kernel[..., :rows_each, :].reshape(krows, chans)
    power = power.astype(jnp.float32) + int(lax.axis_size(AXES)).bit_length() - 15.0
    scale = (jnp.exp2(-power), jnp.exp2(power))

    flat_in = activations.reshape(count, chans)

    def piece(tap):
        f, h, w = tap // 9, tap // 3 % 3, tap % 3
        source = flat if f == 1 else padded[2 - f : 2 - f + frames]
        back = source[:, 2 - h : 2 - h + height, 2 - w : 2 - w + width].reshape(count, chans)
        return lax.dot_general(
            flat_in, back, (((0,), (0,)), ((), ())), preferred_element_type=jnp.float32
        )

    half = krows // 2
    parts = [jnp.zeros((half, chans), jnp.float32) for _ in range(2)]
    for tap in CENTRE_FIRST:
        value = piece(tap)
        for p in range(2):
            low, high = max(tap * chans, p * half), min((tap + 1) * chans, (p + 1) * half)
            if low < high:
                rows = value[low - tap * chans : high - tap * chans]
                parts[p] = lax.dynamic_update_slice(parts[p], rows, (low - p * half, 0))
    sums = []
    for p, way in enumerate(ways):
        terms = [parts[p]]
        for n, stage in enumerate(way):
            terms = halve(terms, stage, scale if n > 0 else None)
        sums.append(sum(terms))
    terms = [jnp.concatenate(sums, 0)]
    for stage in height_bits:
        terms = halve(terms, stage)
    rows = sum(terms)

    gram = lax.dot_general(rows, rows, (((0,), (0,)), ((), ())), precision=HIGHEST)
    for stage in near:
        gram = sum(halve([gram], stage))
    for stage in frame_bits + rest + height_bits:
        gram = gram + swap(gram, stage)
    for stage in near:
        gram = double(gram, stage)

    block = short(rows, scale[0])[None]
    for stage in height_bits[::-1]:
        block = double(block, stage)
    blocks = list(jnp.split(block, 2, 0))
    for p, way in enumerate(ways):
        for stage in way[:0:-1]:
            blocks[p] = double(blocks[p], stage)

    total = lax.conv_general_dilated(
        padded[None],
        full_kernel.reshape(3, 3, 3, chans, chans)[::-1, ::-1, ::-1],
        (1, 1, 1),
        "VALID",
        dimension_numbers=("NDHWC", "DHWIO", "NDHWC"),
        preferred_element_type=jnp.float32,
    )[0]
    input_grad = (total / jnp.sqrt(jnp.float32(krows))).astype(jnp.bfloat16)

    matrix, root = newton_start(gram, damping, ITERS - 4)
    root = newton_end(gram, matrix, root, 4, krows * chans)
    root = root * scale[1]
    new_kernel = jnp.zeros((krows, chans), jnp.bfloat16)
    (stage,) = near
    mine = upper(stage)
    arrived = [swap(block, stage) for block in blocks]
    for group, up in ((blocks, mine), (arrived, 1 - mine)):
        for p, block in enumerate(group):
            offset = p * half + up * (half // 2)
            step = jnp.dot(
                block.reshape(half // 2, chans).astype(jnp.float32), root, precision=lax.Precision.HIGH
            )
            old = lax.dynamic_slice_in_dim(full_kernel, offset, half // 2).astype(jnp.float32)
            new = (old - step).astype(jnp.bfloat16)
            new_kernel = lax.dynamic_update_slice(new_kernel, new, (offset, 0))
    return (input_grad, new_kernel)


def solution(mesh):
    placed = (
        P("frame", "height", "width", None),
        P("frame", "height", "width", None),
        P(("frame", "height", "width"), None),
        P(),
    )
    return jax.shard_map(
        run,
        mesh=mesh,
        in_specs=placed,
        out_specs=(P("frame", "height", "width", None), P()),
        check_vma=False,
    )
```

```python
import jax
import jax.numpy as jnp
from jax import lax
from jax.experimental import pallas as pl
from jax.experimental.pallas import tpu as pltpu
from jax.sharding import PartitionSpec as P

ITERS = 12
CENTRE_FIRST = list(range(9, 18)) + list(range(9)) + list(range(18, 27))
AXES = ("frame", "height", "width")
HIGHEST = lax.Precision.HIGHEST


def bits_of(axis):
    size = lax.axis_size(axis)
    assert size & (size - 1) == 0
    return [(axis, k) for k in range(size.bit_length() - 1)]


def upper(stage):
    axis, k = stage
    return (lax.axis_index(axis) >> k) & 1


def swap(value, stage):
    axis, k = stage
    return lax.ppermute(value, axis, [(i, i ^ (1 << k)) for i in range(lax.axis_size(axis))])


def short(value, scale):
    return (value * scale).astype(jnp.float16)


def halve(terms, stage, scale=None):
    half = terms[0].shape[0] // 2
    up = upper(stage)
    send = sum(lax.dynamic_slice_in_dim(t, (1 - up) * half, half) for t in terms)
    if scale is None:
        got = swap(send, stage)
    else:
        got = swap(short(send, scale[0]), stage).astype(jnp.float32) * scale[1]
    return [lax.dynamic_slice_in_dim(t, up * half, half) for t in terms] + [got]


def double(value, stage):
    got = swap(value, stage)
    up = upper(stage) == 1
    return jnp.concatenate([jnp.where(up, got, value), jnp.where(up, value, got)], 0)


def with_halo(cells, axis, dim):
    count = lax.axis_size(axis)
    head = lax.slice_in_dim(cells, 0, 1, axis=dim)
    tail = lax.slice_in_dim(cells, cells.shape[dim] - 1, cells.shape[dim], axis=dim)
    if count == 2:
        first = lax.axis_index(axis) == 0
        got = lax.ppermute(jnp.where(first, tail, head), axis, [(0, 1), (1, 0)])
        none = jnp.zeros_like(got)
        before, after = jnp.where(first, none, got), jnp.where(first, got, none)
    else:
        before = lax.ppermute(tail, axis, [(i, i + 1) for i in range(count - 1)])
        after = lax.ppermute(head, axis, [(i + 1, i) for i in range(count - 1)])
    return jnp.concatenate([before, cells, after], axis=dim)


def thirds(value):
    high = value.astype(jnp.bfloat16)
    rest = value - high.astype(jnp.float32)
    middle = rest.astype(jnp.bfloat16)
    return high, middle, (rest - middle.astype(jnp.float32)).astype(jnp.bfloat16)


def mul(left, right):
    (a, b, c), (d, e, f) = left, right
    return jnp.dot(
        jnp.concatenate([c, a, b, b, a, a], 1),
        jnp.concatenate([d, f, e, d, e, d], 0),
        preferred_element_type=jnp.float32,
    )


def eye(order):
    rows = lax.broadcasted_iota(jnp.int32, (order, order), 0)
    return (rows == lax.broadcasted_iota(jnp.int32, (order, order), 1)).astype(jnp.float32)


def total_of(value):
    return jnp.sum(jnp.sum(value, 1, keepdims=True), 0, keepdims=True)


def newton_steps(matrix_ref, root_ref, steps):
    order = matrix_ref.shape[0]

    def step(_, carry):
        matrix = matrix_ref[...]
        middle = (5.0 * eye(order) - matrix) / 4.0
        middle = thirds(middle)
        square = thirds(mul(middle, middle))
        inner = thirds(mul(square, thirds(matrix)))
        root_ref[...] = mul(thirds(root_ref[...]), middle)
        matrix_ref[...] = mul(square, inner)
        return carry

    lax.fori_loop(0, steps, step, 0)


def newton_start(gram, damping, steps):
    order = gram.shape[0]

    def body(damping_ref, gram_ref, matrix_ref, root_ref):
        gram = gram_ref[...]
        identity = eye(order)
        factor = gram + damping_ref[0, 0] * (total_of(gram * identity) / order) * identity
        scale = 2.5 / jnp.sqrt(total_of(factor * factor))
        root_ref[...] = jnp.sqrt(jnp.sqrt(scale)) * identity
        matrix_ref[...] = scale * factor
        newton_steps(matrix_ref, root_ref, steps)

    shape = jax.ShapeDtypeStruct(gram.shape, jnp.float32)
    return pl.pallas_call(
        body,
        in_specs=[pl.BlockSpec(memory_space=pltpu.SMEM), pl.BlockSpec(memory_space=pltpu.VMEM)],
        out_shape=(shape, shape),
        cost_estimate=pl.CostEstimate(flops=48 * steps * order**3, transcendentals=0, bytes_accessed=12 * order**2),
    )(damping.reshape(1, 1), gram)


def newton_end(gram, matrix, root, steps, entries):
    order = gram.shape[0]

    def body(gram_ref, matrix_in, root_in, out_ref, matrix_ref, root_ref):
        matrix_ref[...] = matrix_in[...]
        root_ref[...] = root_in[...]
        newton_steps(matrix_ref, root_ref, steps)
        root = root_ref[...]
        size = jnp.sqrt(total_of(root * mul(thirds(gram_ref[...]), thirds(root))) / entries + 1e-06)
        out_ref[...] = root * (0.5 / size)

    shape = jax.ShapeDtypeStruct(gram.shape, jnp.float32)
    return pl.pallas_call(
        body,
        out_shape=shape,
        scratch_shapes=[pltpu.VMEM(gram.shape, jnp.float32)] * 2,
        cost_estimate=pl.CostEstimate(flops=48 * steps * order**3, transcendentals=0, bytes_accessed=16 * order**2),
    )(gram, matrix, root)


def run(activations, out_grad, kernel, damping):
    frames, height, width, chans = activations.shape
    count = frames * height * width
    near = bits_of("width")[:1]
    rest = bits_of("width")[1:]
    frame_bits, height_bits = bits_of("frame"), bits_of("height")
    rows_each = kernel.shape[0]
    krows = rows_each * lax.axis_size(AXES)
    ways = [near + frame_bits + rest, near + rest + frame_bits]

    flat = with_halo(with_halo(out_grad, "height", 1), "width", 2)
    padded = with_halo(flat, "frame", 0)

    top = jnp.max(jnp.abs(activations)).astype(jnp.float32) * jnp.max(jnp.abs(out_grad)).astype(jnp.float32)
    power = jnp.ceil(jnp.log2(jnp.maximum(top * count, 1e-30))).astype(jnp.bfloat16)
    extra = 16 - rows_each % 16
    tall = rows_each + extra
    gathered = jnp.concatenate([kernel, jnp.full((extra, chans), power, jnp.bfloat16)], 0)[None]
    for stage in height_bits[::-1]:
        gathered = double(gathered, stage)
    sides = []
    for p, way in enumerate(ways):
        side = gathered[..., p * (chans // 2) : (p + 1) * (chans // 2)]
        for stage in way[:0:-1]:
            side = double(side, stage)
        order = way[1:] + height_bits
        want = frame_bits + height_bits[::-1] + rest[::-1]
        side = side.reshape((2,) * len(order) + side.shape[1:])
        axes = [order.index(s) for s in want] + [len(order), len(order) + 1]
        sides.append(side.transpose(axes).reshape(-1, tall, chans // 2))
    full_kernel = jnp.concatenate(sides, 2)
    power = jnp.max(full_kernel[:, rows_each, 0])
    for stage in near:
        got = swap(full_kernel, stage)
        power = jnp.maximum(power, jnp.max(got[:, rows_each, 0]))
        up = upper(stage) == 1
        full_kernel = jnp.stack([jnp.where(up, got, full_kernel), jnp.where(up, full_kernel, got)], 1)
    full_kernel = full_kernel[..., :rows_each, :].reshape(krows, chans)
    power = power.astype(jnp.float32) + int(lax.axis_size(AXES)).bit_length() - 15.0
    scale = (jnp.exp2(-power), jnp.exp2(power))

    flat_in = activations.reshape(count, chans)

    def piece(tap):
        f, h, w = tap // 9, tap // 3 % 3, tap % 3
        source = flat if f == 1 else padded[2 - f : 2 - f + frames]
        back = source[:, 2 - h : 2 - h + height, 2 - w : 2 - w + width].reshape(count, chans)
        return lax.dot_general(
            flat_in, back, (((0,), (0,)), ((), ())), preferred_element_type=jnp.float32
        )

    half = krows // 2
    parts = [jnp.zeros((half, chans), jnp.float32) for _ in range(2)]
    for tap in CENTRE_FIRST:
        value = piece(tap)
        for p in range(2):
            low, high = max(tap * chans, p * half), min((tap + 1) * chans, (p + 1) * half)
            if low < high:
                rows = value[low - tap * chans : high - tap * chans]
                parts[p] = lax.dynamic_update_slice(parts[p], rows, (low - p * half, 0))
    sums = []
    for p, way in enumerate(ways):
        terms = [parts[p]]
        for n, stage in enumerate(way):
            terms = halve(terms, stage, scale if n > 0 else None)
        sums.append(sum(terms))
    terms = [jnp.concatenate(sums, 0)]
    for stage in height_bits:
        terms = halve(terms, stage)
    rows = sum(terms)

    gram = lax.dot_general(rows, rows, (((0,), (0,)), ((), ())), precision=HIGHEST)
    for stage in near:
        gram = sum(halve([gram], stage))
    for stage in frame_bits + rest + height_bits:
        gram = gram + swap(gram, stage)
    for stage in near:
        gram = double(gram, stage)

    block = short(rows, scale[0])[None]
    for stage in height_bits[::-1]:
        block = double(block, stage)
    blocks = list(jnp.split(block, 2, 0))
    for p, way in enumerate(ways):
        for stage in way[:0:-1]:
            blocks[p] = double(blocks[p], stage)

    total = lax.conv_general_dilated(
        padded[None],
        full_kernel.reshape(3, 3, 3, chans, chans)[::-1, ::-1, ::-1],
        (1, 1, 1),
        "VALID",
        dimension_numbers=("NDHWC", "DHWIO", "NDHWC"),
        preferred_element_type=jnp.float32,
    )[0]
    input_grad = (total / jnp.sqrt(jnp.float32(krows))).astype(jnp.bfloat16)

    matrix, root = newton_start(gram, damping, ITERS - 4)
    root = newton_end(gram, matrix, root, 4, krows * chans)
    root = root * scale[1]
    new_kernel = jnp.zeros((krows, chans), jnp.bfloat16)
    (stage,) = near
    mine = upper(stage)
    arrived = [swap(block, stage) for block in blocks]
    for group, up in ((blocks, mine), (arrived, 1 - mine)):
        for p, block in enumerate(group):
            offset = p * half + up * (half // 2)
            step = jnp.dot(
                block.reshape(half // 2, chans).astype(jnp.float32), root, precision=lax.Precision.HIGH
            )
            old = lax.dynamic_slice_in_dim(full_kernel, offset, half // 2).astype(jnp.float32)
            new = (old - step).astype(jnp.bfloat16)
            new_kernel = lax.dynamic_update_slice(new_kernel, new, (offset, 0))
    return (input_grad, new_kernel)


def solution(mesh):
    placed = (
        P("frame", "height", "width", None),
        P("frame", "height", "width", None),
        P(("frame", "height", "width"), None),
        P(),
    )
    return jax.shard_map(
        run,
        mesh=mesh,
        in_specs=placed,
        out_specs=(P("frame", "height", "width", None), P()),
        check_vma=False,
    )
```
